32 devices in a mesh: fsdp: 8 (over z, x), dp: 4 (over y, core).
Axes of the slice: x: 2, y: 2, z: 4, core: 2. Of those that a mesh axis runs over, the one named last changes fastest.
Arguments:
- inputs: bfloat16 [32768, 768], P(('fsdp', 'dp')), may hold values from -6 to 6
- row_ids: int32 [32768], P(('fsdp', 'dp')), may hold values from 0 to 7, as said below
- ln_gains: bfloat16 [2, 768], P(None, 'fsdp'), may hold values from 0.099609375 to 1.8984375
- biases: bfloat16 [6, 768], P(None, 'fsdp'), may hold values from -3 to 3
- w_qkv: bfloat16 [768, 2304], P('fsdp'), may hold values from -0.21875 to 0.21875
- w_out: bfloat16 [768, 768], P('fsdp'), may hold values from -0.75 to 0.75
- w_up: bfloat16 [768, 3072], P('fsdp'), may hold values from -0.21875 to 0.21875
- bias_up: bfloat16 [3072], P('fsdp'), may hold values from -3 to 3
- w_down: bfloat16 [3072, 768], P('fsdp'), may hold values from -0.109375 to 0.109375
- cotangent: bfloat16 [32768, 768], P(('fsdp', 'dp')), may hold values from -6 to 6
Outputs:
- block_out: bfloat16 [32768, 768], P(('fsdp', 'dp'))
- d_inputs: float32 [32768, 768], P(('fsdp', 'dp'))
- g_ln_gains: float32 [2, 768], P(None, 'fsdp')
- g_biases: float32 [6, 768], P(None, 'fsdp')
- g_w_qkv: float32 [768, 2304], P('fsdp')
- g_w_out: float32 [768, 768], P('fsdp')
- g_w_up: float32 [768, 3072], P('fsdp')
- g_bias_up: float32 [3072], P('fsdp')
- g_w_down: float32 [3072, 768], P('fsdp')
The draws below stay inside these ranges and needn't reach their ends.
Inputs may be any that keep to these rules, and one draw needn't show every extreme that they name: `row_ids`: on each device the 1024 tokens form rows of 128 or 256 consecutive tokens, the longer rows first, so that each row starts at a multiple of its own length; the value numbers a token's row on its device from 0 in order; some device holds only rows of 128.
All inputs are finite; a program needn't handle non-finite values.
Results may differ from the reference program's by a relative error of at most 0.011.
Values may be sent and summed in bfloat16 or wider, within the bound.
A program may use at most 256 MiB of HBM per device.

```python
import math
import jax
import jax.numpy as jnp
from jax import lax

D = 768
HEADS = 12
HEAD = 64
FF = 3072
TOK_DEV = 1024
SHORT = 128
TOKENS = 32768


def draw_row_ids(key, part):
    device_count = TOKENS // TOK_DEV
    most_long = TOK_DEV // (2 * SHORT)
    first_key, second_key = jax.random.split(key)
    long_rows = jax.random.randint(first_key, (device_count,), 0, most_long + 1)
    chosen = jax.random.randint(second_key, (), 0, device_count)
    long_rows = jnp.where(jnp.arange(device_count) == chosen, 0, long_rows)
    position = jnp.arange(TOK_DEV)[None, :]
    boundary = long_rows[:, None] * (2 * SHORT)
    row_numbers = jnp.where(position < boundary, position // (2 * SHORT), long_rows[:, None] + (position - boundary) // SHORT)
    return row_numbers.reshape(TOKENS).astype(jnp.int32)


def shard_levels(stream_key, extent, pieces, smallest, top_value):
    def one(dim, blocks):
        heights = jax.random.uniform(jax.random.fold_in(jax.random.fold_in(stream_key, 6), dim), (blocks,), jnp.float32, smallest / len(pieces), top_value / len(pieces))
        return jnp.repeat(jnp.exp(heights), extent[dim] // blocks).reshape((-1,) + (1,) * (len(extent) - dim - 1))

    factor_of = one(*pieces[0])
    for cut in pieces[1:]:
        factor_of = factor_of * one(*cut)
    return factor_of


def centred(stream_key, extent, scale, limit, cuts=(), dtype=jnp.bfloat16):
    values = scale * jax.random.normal(stream_key, extent, jnp.float32)
    if cuts:
        values = values * shard_levels(stream_key, extent, cuts, -0.22, 0.18)
    return jnp.clip(values, -limit, limit).astype(dtype)


def setup_inputs(seed: int = 0) -> dict:
    streams_of = jax.random.split(jax.random.key(seed), 11)
    return {
        "inputs": centred(streams_of[0], (TOKENS, D), 1.0, 6.0, ((0, 32),)),
        "row_ids": draw_row_ids(jax.random.fold_in(streams_of[10], 71), 0),
        "ln_gains": jnp.clip(1.0 + 0.18 * jax.random.normal(streams_of[2], (2, D), jnp.float32), 0.099609375, 1.8984375).astype(jnp.bfloat16),
        "biases": centred(streams_of[3], (6, D), 0.5, 3.0, ((1, 8),)),
        "w_qkv": centred(streams_of[4], (D, 3 * D), D ** -0.5, 0.21875, ((0, 8),)),
        "w_out": centred(streams_of[5], (D, D), (D // 12) ** -0.5, 0.75, ((0, 8),)),
        "w_up": centred(streams_of[6], (D, FF), D ** -0.5, 0.21875, ((0, 8),)),
        "bias_up": centred(streams_of[7], (FF,), 0.5, 3.0, ((0, 8),)),
        "w_down": centred(streams_of[8], (FF, D), FF ** -0.5, 0.109375, ((0, 8),)),
        "cotangent": centred(streams_of[9], (TOKENS, D), 1.0, 6.0, ((0, 32),)),
    }


@jax.custom_vjp
def low(v):
    return lax.optimization_barrier(v.astype(jnp.bfloat16)).astype(jnp.float32)

@jax.custom_vjp
def low_back(v):
    return v

def low_keep(v):
    return (low(v), None)

def low_pass(kept, grad):
    return (grad,)

def back_keep(v):
    return (v, None)

def back_low(kept, grad):
    return (low(grad),)
low.defvjp(low_keep, low_pass)
low_back.defvjp(back_keep, back_low)
norm_eps = 1e-05

def layer_norm(values, gain, shift):
    center = values - lax.optimization_barrier(jnp.mean(values, axis=-1, keepdims=True))
    spread = lax.optimization_barrier(jnp.mean(center * center, axis=-1, keepdims=True))
    return center * lax.rsqrt(spread + norm_eps) * gain + shift

def gelu_tanh(values):
    inner = math.sqrt(2.0 / math.pi) * (values + 0.044715 * values * values * values)
    return 0.5 * values * (1.0 + jnp.tanh(inner))

def product(left, right):
    return jnp.dot(left, right, precision=lax.Precision.HIGHEST, preferred_element_type=jnp.float32)

def attend(group):
    query, keys, values, row_numbers = group
    count_rows = query.shape[0]
    query_heads = query.reshape(count_rows, HEADS, HEAD)
    key_heads = keys.reshape(count_rows, HEADS, HEAD)
    value_heads = values.reshape(count_rows, HEADS, HEAD)
    raw_scores = jnp.einsum('qhd,khd->hqk', query_heads, key_heads, precision=lax.Precision.HIGHEST)
    scores = low_back(raw_scores * (1.0 / math.sqrt(HEAD)))
    same_row = row_numbers[:, None] == row_numbers[None, :]
    scores = jnp.where(same_row[None], scores, -1000000000.0)
    row_max = lax.optimization_barrier(jnp.max(scores, axis=-1, keepdims=True))
    exponent = jnp.exp(scores - row_max)
    attn_probs = low(exponent / lax.optimization_barrier(jnp.sum(exponent, axis=-1, keepdims=True)))
    result = jnp.einsum('hqk,khd->qhd', attn_probs, value_heads, precision=lax.Precision.HIGHEST)
    return result.reshape(count_rows, HEADS * HEAD)

def forward(tokens, gains, shifts, w_qkv, w_out, w_up, bias_up, w_down, row_ids):
    normed = low(layer_norm(tokens, gains[0], shifts[0]))
    qkv_bias = jnp.concatenate([shifts[1], jnp.zeros_like(shifts[1]), shifts[2]])
    qkv = low(low_back(product(normed, w_qkv) + qkv_bias))
    grouped = qkv.reshape(-1, TOK_DEV, 3 * D)
    mixed = lax.map(jax.checkpoint(attend), (grouped[:, :, :D], grouped[:, :, D:2 * D], grouped[:, :, 2 * D:], row_ids.reshape(-1, TOK_DEV)))
    mixed = low(low_back(mixed.reshape(-1, D)))
    middle = tokens + low_back(product(mixed, w_out)) + shifts[3]
    normed_two = low(layer_norm(middle, gains[1], shifts[4]))
    upper = low_back(product(normed_two, w_up) + bias_up)
    hidden = low(gelu_tanh(upper))
    return middle + low_back(product(hidden, w_down)) + shifts[5]

def reference(inputs, row_ids, ln_gains, biases, w_qkv, w_out, w_up, bias_up, w_down, cotangent):
    floats = [a.astype(jnp.float32) for a in (inputs, ln_gains, biases, w_qkv, w_out, w_up, bias_up, w_down)]

    def apply_block(tokens, gains, shifts, wq, wo, wu, bu, wd):
        return forward(tokens, gains, shifts, wq, wo, wu, bu, wd, row_ids)
    result, pull = jax.vjp(apply_block, *floats)
    grads = pull(cotangent.astype(jnp.float32))
    return (result.astype(jnp.bfloat16), grads[0], grads[1], grads[2], grads[3], grads[4], grads[5], grads[6], grads[7])
```

```python
import functools
import math

import jax
import jax.numpy as jnp
from jax import lax
from jax.experimental import pallas as pl
from jax.experimental.pallas import tpu as pltpu
from jax.sharding import PartitionSpec as P

MESH = pl.DeviceIdType.MESH
F32 = jnp.float32
BF16 = jnp.bfloat16


class Place:
    def __init__(self):
        f = lax.axis_index("fsdp")
        d = lax.axis_index("dp")
        self.f, self.d = f, d
        self.z, self.x = f // 2, f % 2
        self.y, self.c = d // 2, d % 2

    def at(self, z=None, x=None, y=None, c=None):
        z = self.z if z is None else z
        x = self.x if x is None else x
        y = self.y if y is None else y
        c = self.c if c is None else c
        return (z * 2 + x, y * 2 + c)

    def z_to(self, k):
        return (self.z + k) % 4

    def z_from(self, k):
        return (self.z + 4 - k) % 4


def copy_to(src, dst, send, recv, device):
    return pltpu.make_async_remote_copy(
        src_ref=src, dst_ref=dst, send_sem=send, recv_sem=recv, device_id=device, device_id_type=MESH
    )


def greet(place):
    barrier = pltpu.get_barrier_semaphore()
    others = [place.at(z=place.z_to(k)) for k in (1, 2, 3)]
    others += [place.at(z=place.z_to(k), x=1 - place.x) for k in (0, 1, 2, 3)]
    others += [place.at(y=1 - place.y), place.at(c=1 - place.c)]
    for other in others:
        pl.semaphore_signal(barrier, inc=1, device_id=other, device_id_type=MESH)
    pl.semaphore_wait(barrier, len(others))


class Gather:
    def __init__(self, place, chunks, send, recv):
        self.p, self.chunks, self.send, self.recv = place, chunks, send, recv
        self.sent = []

    def view(self, k, f, start, width):
        src, full, rows, row, col = self.chunks[k]
        return full.at[pl.ds(pl.multiple_of(f * rows + row, 32), 96), pl.ds(pl.multiple_of(col + start, 128), width)]

    def own(self, k, start, width):
        src, full, rows, row, col = self.chunks[k]
        return src.at[pl.ds(row, 96), pl.ds(pl.multiple_of(col + start, 128), width)]

    def put(self, k, slot, src, dst, device):
        copy = copy_to(src, dst, self.send.at[k, slot], self.recv.at[k, slot], device)
        copy.start()
        self.sent.append(copy)

    def got(self, k, slot, dst):
        copy_to(dst, dst, self.send.at[k, slot], self.recv.at[k, slot], self.p.at(c=1 - self.p.c)).wait_recv()

    def ab(self):
        return self.p.c * 384 + self.p.y * 128

    def mine(self):
        return self.p.c * 384 + self.p.y * 256

    def theirs(self):
        return self.p.c * 384 + (1 - self.p.y) * 256

    def half(self):
        return self.p.c * 384

    def start(self, k):
        p = self.p
        src = self.own(k, self.ab(), 256)
        dst = self.view(k, p.f, self.ab(), 256)
        for hop in (1, 2, 3):
            self.put(k, hop - 1, src, dst, p.at(z=p.z_to(hop)))
        self.put(k, 3, src, dst, p.at(x=1 - p.x))

    def z_event(self, k, hop):
        p = self.p
        f = p.z_from(hop) * 2 + p.x
        ab = self.view(k, f, self.ab(), 256)
        self.got(k, hop - 1, ab)
        self.put(k, 3 + hop, ab, ab, p.at(x=1 - p.x))
        b = self.view(k, f, self.mine(), 128)
        self.put(k, 7 + hop - 1, b, b, p.at(y=1 - p.y))

    def x_event(self, k, hop):
        p = self.p
        f = p.z_from(hop) * 2 + 1 - p.x
        self.got(k, 3 + hop, self.view(k, f, self.ab(), 256))
        b = self.view(k, f, self.mine(), 128)
        self.put(k, 10 + hop, b, b, p.at(y=1 - p.y))

    def source(self, j):
        p = self.p
        return p.z_from(j + 1) * 2 + p.x if j < 3 else p.z_from(j - 3) * 2 + 1 - p.x

    def y_event(self, k, j):
        p = self.p
        f = self.source(j)
        self.got(k, 7 + j, self.view(k, f, self.theirs(), 128))
        h = self.view(k, f, self.half(), 384)
        self.put(k, 14 + j, h, h, p.at(c=1 - p.c))

    def c_event(self, k, j):
        p = self.p
        self.got(k, 14 + j, self.view(k, self.source(j), (1 - p.c) * 384, 384))

    def finish(self):
        for copy in self.sent:
            copy.wait_send()


class Reduce:
    def __init__(self, place, k, grads, bufs, final, send, recv):
        self.p, self.k, self.g, self.b, self.out = place, k, grads, bufs, final
        self.send, self.recv = send, recv
        self.sent = []
        self.slot_a = 3 * place.c + 1
        self.slot_b = 3 * place.c + 2 * place.y
        self.slot_o = 3 * place.c + 2 * (1 - place.y)

    def put(self, s, src, dst, device):
        copy = copy_to(src, dst, self.send.at[self.k, s], self.recv.at[self.k, s], device)
        copy.start()
        self.sent.append(copy)

    def got(self, s, dst):
        copy_to(dst, dst, self.send.at[self.k, s], self.recv.at[self.k, s], self.p.at(c=1 - self.p.c)).wait_recv()

    def add(self, dst, src):
        dst[...] = (dst[...].astype(F32) + src[...].astype(F32)).astype(BF16)

    def e0(self):
        p = self.p
        self.put(0, self.g.at[pl.ds(3 * (1 - p.c), 3)], self.b["c"], p.at(c=1 - p.c))

    def e1(self):
        p = self.p
        self.got(0, self.b["c"])
        base = 3 * p.c

        def body(i, _):
            s, z = i // 4, i % 4
            for x in (0, 1):
                self.add(self.g.at[base + s, z, x], self.b["c"].at[s, z, x])
            return 0

        lax.fori_loop(0, 12, body, 0)
        self.put(1, self.g.at[3 * p.c + 2 * (1 - p.y)], self.b["y"], p.at(y=1 - p.y))
        self.put(2, self.g.at[self.slot_a, :, 1 - p.x], self.b["xa"], p.at(x=1 - p.x))

    def x_add(self, slot, s, buf):
        p = self.p
        self.got(s, buf)

        def body(z, _):
            self.add(self.g.at[slot, z, p.x], buf.at[z])
            return 0

        lax.fori_loop(0, 4, body, 0)

    def z_put(self, slot, s, buf):
        p = self.p
        for hop in (1, 2, 3):
            z = p.z_to(hop)
            self.put(s + hop - 1, self.g.at[slot, z, p.x], buf.at[hop - 1], p.at(z=z))

    def z_sum(self, slot, s, buf):
        p = self.p
        total = self.g[slot, p.z, p.x].astype(F32)
        for hop in (1, 2, 3):
            self.got(s + hop - 1, buf.at[hop - 1])
            total = total + buf[hop - 1].astype(F32)
        return total.astype(BF16)

    def e2(self):
        self.x_add(self.slot_a, 2, self.b["xa"])
        self.z_put(self.slot_a, 3, self.b["za"])

    def e3(self):
        p = self.p
        self.got(1, self.b["y"])

        def body(z, _):
            for x in (0, 1):
                self.add(self.g.at[self.slot_b, z, x], self.b["y"].at[z, x])
            return 0

        lax.fori_loop(0, 4, body, 0)
        self.put(6, self.g.at[self.slot_b, :, 1 - p.x], self.b["xb"], p.at(x=1 - p.x))

    def e4(self):
        p = self.p
        self.b["pa"][...] = self.z_sum(self.slot_a, 3, self.b["za"])
        self.put(7, self.b["pa"], self.b["ya"], p.at(y=1 - p.y))

    def e5(self):
        self.x_add(self.slot_b, 6, self.b["xb"])
        self.z_put(self.slot_b, 8, self.b["zb"])

    def e6(self):
        p = self.p
        self.out[self.slot_b] = self.z_sum(self.slot_b, 8, self.b["zb"])
        self.put(11, self.out.at[self.slot_b], self.out.at[self.slot_b], p.at(y=1 - p.y))

    def e7(self):
        self.got(7, self.b["ya"])
        self.out[self.slot_a] = (self.b["pa"][...].astype(F32) + self.b["ya"][...].astype(F32)).astype(BF16)

    def e8(self):
        p = self.p
        self.got(11, self.out.at[self.slot_o])
        half = self.out.at[pl.ds(3 * p.c, 3)]
        self.put(12, half, half, p.at(c=1 - p.c))

    def e9(self):
        self.got(12, self.out.at[pl.ds(3 * (1 - self.p.c), 3)])

    def finish(self):
        for copy in self.sent:
            copy.wait_send()

    def events(self):
        return [self.e0, self.e1, self.e2, self.e3, self.e4, self.e5, self.e6, self.e7, self.e8, self.e9]


def reduce_bufs(r, w):
    v = lambda *lead: pltpu.VMEM((*lead, r, w), BF16)
    return dict(c=v(3, 4, 2), y=v(4, 2), xa=v(4), xb=v(4), za=v(3), zb=v(3), pa=v(), ya=v())


BUF_NAMES = ("c", "y", "xa", "xb", "za", "zb", "pa", "ya")


def gather_kernel(q_ref, o_ref, u_ref, d_ref, fq, fo, fu, fd, send, recv, local):
    p = Place()
    chunks = [(q_ref, fq, 96, 0, 768 * j) for j in range(3)]
    chunks += [(o_ref, fo, 96, 0, 0)]
    chunks += [(u_ref, fu, 96, 0, 768 * j) for j in range(4)]
    chunks += [(d_ref, fd, 384, 96 * j, 0) for j in range(4)]
    g = Gather(p, chunks, send, recv)
    greet(p)
    owns = []
    for i, (src, dst, rows) in enumerate(((q_ref, fq, 96), (o_ref, fo, 96), (u_ref, fu, 96), (d_ref, fd, 384))):
        copy = pltpu.make_async_copy(src, dst.at[pl.ds(pl.multiple_of(p.f * rows, 32), rows)], local.at[i])
        copy.start()
        owns.append(copy)
    n = len(chunks)
    stages = 5
    for t in range(n + stages - 1):
        for stage in range(stages):
            k = t - stage
            if not 0 <= k < n:
                continue
            if stage == 0:
                g.start(k)
            elif stage == 1:
                for hop in (1, 2, 3):
                    g.z_event(k, hop)
            elif stage == 2:
                for hop in (0, 1, 2, 3):
                    g.x_event(k, hop)
            elif stage == 3:
                for j in range(7):
                    g.y_event(k, j)
            else:
                for j in range(7):
                    g.c_event(k, j)
    for copy in owns:
        copy.wait()
    g.finish()


def gather_weights(w_qkv, w_out, w_up, w_down):
    args = (w_qkv, w_out, w_up, w_down)
    hbm = pl.BlockSpec(memory_space=pl.ANY)
    vmem = pl.BlockSpec(memory_space=pltpu.VMEM)
    return pl.pallas_call(
        gather_kernel,
        out_shape=[jax.ShapeDtypeStruct((a.shape[0] * 8, a.shape[1]), BF16) for a in args],
        in_specs=[hbm] * 4,
        out_specs=[vmem] * 4,
        scratch_shapes=[
            pltpu.SemaphoreType.DMA((12, 21)),
            pltpu.SemaphoreType.DMA((12, 21)),
            pltpu.SemaphoreType.DMA((4,)),
        ],
        compiler_params=pltpu.CompilerParams(
            collective_id=0, has_side_effects=True, vmem_limit_bytes=60 << 20
        ),
        name="gather",
    )(*args)


def reduce_kernel(d_ref, u_ref, o_ref, q_ref, od, ou, oo, oq, gd, gu, go, gq, fd, fx, *rest):
    nb = len(BUF_NAMES)
    bd = [dict(zip(BUF_NAMES, rest[:nb]))]
    bx = dict(zip(BUF_NAMES, rest[nb : 2 * nb]))
    send, recv, local = rest[2 * nb :]
    p = Place()
    sel = lambda bufs, j: {n: r.at[j] for n, r in bufs.items()}
    chunks = []
    loads = []
    for j in range(3):
        chunks.append(Reduce(p, j, gd.at[j], sel(bd[0], j), fd.at[j], send, recv))
        for s in range(6):
            loads.append((d_ref.at[:, :, s, :, pl.ds(256 * j, 256)], gd.at[j, s]))
    for j in range(4):
        chunks.append(Reduce(p, 3 + j, gu.at[j], sel(bx, j), fx.at[j], send, recv))
        for s in range(6):
            loads.append((u_ref.at[:, :, :, pl.ds(768 * j + 128 * s, 128)], gu.at[j, s]))
    chunks.append(Reduce(p, 7, go.at[0], sel(bx, 4), fx.at[4], send, recv))
    for s in range(6):
        loads.append((o_ref.at[:, :, :, pl.ds(128 * s, 128)], go.at[0, s]))
    for j in range(3):
        chunks.append(Reduce(p, 8 + j, gq.at[j], sel(bx, 5 + j), fx.at[5 + j], send, recv))
        for s in range(6):
            col = (s // 2) * 768 + 256 * j + 128 * (s % 2)
            loads.append((q_ref.at[:, :, :, pl.ds(col, 128)], gq.at[j, s]))
    copies = [pltpu.make_async_copy(a, b, local.at[i]) for i, (a, b) in enumerate(loads)]
    for copy in copies:
        copy.start()
    greet(p)
    for copy in copies:
        copy.wait()
    n = len(chunks)
    for t in range(n + 9):
        for stage in range(9, -1, -1):
            k = t - stage
            if 0 <= k < n:
                chunks[k].events()[stage]()
    for chunk in chunks:
        chunk.finish()
    for j in range(3):
        for s in range(6):
            od[64 * s : 64 * s + 64, 256 * j : 256 * j + 256] = fd[j, s]
    for j in range(4):
        for s in range(6):
            ou[:, 768 * j + 128 * s : 768 * j + 128 * s + 128] = fx[j, s]
    for s in range(6):
        oo[:, 128 * s : 128 * s + 128] = fx[4, s]
    for j in range(3):
        for s in range(6):
            col = (s // 2) * 768 + 256 * j + 128 * (s % 2)
            oq[:, col : col + 128] = fx[5 + j, s]


def reduce_grads(gd, gu, go, gq):
    hbm = pl.BlockSpec(memory_space=pl.ANY)
    vmem = pl.BlockSpec(memory_space=pltpu.VMEM)
    gd = gd.reshape(4, 2, 6, 64, 768)
    gu = gu.reshape(4, 2, 96, 3072)
    go = go.reshape(4, 2, 96, 768)
    gq = gq.reshape(4, 2, 96, 2304)
    lead = lambda n, r, w: [
        pltpu.VMEM((n, *b.shape), BF16) for b in (reduce_bufs(r, w)[name] for name in BUF_NAMES)
    ]
    shapes = [(384, 768), (96, 3072), (96, 768), (96, 2304)]
    return pl.pallas_call(
        reduce_kernel,
        out_shape=[jax.ShapeDtypeStruct(s, BF16) for s in shapes],
        in_specs=[hbm] * 4,
        out_specs=[vmem] * 4,
        scratch_shapes=[
            pltpu.VMEM((3, 6, 4, 2, 64, 256), BF16),
            pltpu.VMEM((4, 6, 4, 2, 96, 128), BF16),
            pltpu.VMEM((1, 6, 4, 2, 96, 128), BF16),
            pltpu.VMEM((3, 6, 4, 2, 96, 128), BF16),
            pltpu.VMEM((3, 6, 64, 256), BF16),
            pltpu.VMEM((8, 6, 96, 128), BF16),
            *lead(3, 64, 256),
            *lead(8, 96, 128),
            pltpu.SemaphoreType.DMA((11, 13)),
            pltpu.SemaphoreType.DMA((11, 13)),
            pltpu.SemaphoreType.DMA((66,)),
        ],
        compiler_params=pltpu.CompilerParams(
            collective_id=1, has_side_effects=True, vmem_limit_bytes=60 << 20
        ),
        name="reduce",
    )(gd, gu, go, gq)


HEADS = 12
HEAD = 64
BLOCK = 512


norm_eps = 1e-05


def layer_norm(values, gain, shift):
    center = values - jnp.mean(values, axis=-1, keepdims=True)
    spread = jnp.mean(center * center, axis=-1, keepdims=True)
    return center * lax.rsqrt(spread + norm_eps) * gain + shift


def gelu_tanh(values):
    inner = math.sqrt(2.0 / math.pi) * (values + 0.044715 * values * values * values)
    return 0.5 * values * (1.0 + jnp.tanh(inner))


def contract_rows(left, right):
    return lax.dot_general(
        left, right, (((0,), (0,)), ((), ())), preferred_element_type=jnp.float32
    )


def contract_cols(left, right):
    return lax.dot_general(
        left, right, (((1,), (1,)), ((), ())), preferred_element_type=jnp.float32
    )


def split_heads(values):
    return values.reshape(values.shape[0], HEADS, values.shape[1] // HEADS)


def block_scores(query, keys, query_rows, key_rows):
    raw_scores = jnp.einsum(
        "qhd,khd->hqk", split_heads(query), split_heads(keys), preferred_element_type=jnp.float32
    )
    raw_scores = raw_scores * (1.0 / math.sqrt(HEAD))
    same_row = (query_rows[:, None] == key_rows[None, :])[None]
    return jnp.where(same_row, raw_scores, -1000000000.0)


def attend_forward(query, keys, values, query_rows, key_rows):
    scores = block_scores(query, keys, query_rows, key_rows)
    row_max = jnp.max(scores, axis=-1, keepdims=True)
    exponent = jnp.exp(scores - row_max)
    row_sum = jnp.sum(exponent, axis=-1, keepdims=True)
    attn_probs = (exponent / row_sum).astype(jnp.bfloat16)
    result = jnp.einsum(
        "hqk,khd->qhd", attn_probs, split_heads(values), preferred_element_type=jnp.float32
    )
    return (result.reshape(query.shape[0], -1), (row_max + jnp.log(row_sum))[..., 0])


def attend_backward(query, keys, values, query_rows, key_rows, log_sums, grad_out):
    scores = block_scores(query, keys, query_rows, key_rows)
    attn_probs = jnp.exp(scores - log_sums[..., None])
    probs_low = attn_probs.astype(jnp.bfloat16)
    grad_heads = split_heads(grad_out)
    d_values = jnp.einsum("hqk,qhd->khd", probs_low, grad_heads, preferred_element_type=jnp.float32)
    d_probs = jnp.einsum(
        "qhd,khd->hqk", grad_heads, split_heads(values), preferred_element_type=jnp.float32
    )
    inner = jnp.sum(attn_probs * d_probs, axis=-1, keepdims=True)
    d_scores = (attn_probs * (d_probs - inner)).astype(jnp.bfloat16)
    scale = 1.0 / math.sqrt(HEAD)
    d_query = (
        jnp.einsum("hqk,khd->qhd", d_scores, split_heads(keys), preferred_element_type=jnp.float32)
        * scale
    )
    d_keys = (
        jnp.einsum("hqk,qhd->khd", d_scores, split_heads(query), preferred_element_type=jnp.float32)
        * scale
    )
    return (
        d_query.reshape(query.shape[0], -1),
        d_keys.reshape(keys.shape[0], -1),
        d_values.reshape(keys.shape[0], -1),
    )


def per_device(fast, inputs, row_ids, ln_gains, biases, w_qkv, w_out, w_up, bias_up, w_down, cotangent):
    weights = (w_qkv, w_out, w_up, w_down)
    if fast:
        whole = gather_weights(*weights)
    else:
        whole = [lax.all_gather(a, "fsdp", axis=0, tiled=True) for a in weights]
    gathered = (
        lax.all_gather(ln_gains, "fsdp", axis=1, tiled=True),
        lax.all_gather(biases, "fsdp", axis=1, tiled=True),
        whole[0],
        whole[1],
        whole[2],
        lax.all_gather(bias_up, "fsdp", axis=0, tiled=True),
        whole[3],
    )
    gains = gathered[0].astype(jnp.float32)
    shifts = gathered[1].astype(jnp.float32)
    full_qkv, full_out, full_up, full_bias_up, full_down = (
        gathered[2],
        gathered[3],
        gathered[4],
        gathered[5],
        gathered[6],
    )
    width = full_out.shape[0]
    rows_n = inputs.shape[0]
    blocks_n = rows_n // BLOCK
    tokens_f = inputs.astype(jnp.float32)
    normed_f, norm_pull = jax.vjp(layer_norm, tokens_f, gains[0], shifts[0])
    normed = normed_f.astype(jnp.bfloat16)
    qkv_bias = jnp.concatenate([shifts[1], jnp.zeros_like(shifts[1]), shifts[2]])
    qkv = (jnp.dot(normed, full_qkv, preferred_element_type=jnp.float32) + qkv_bias).astype(
        jnp.bfloat16
    )
    query = qkv[:, :width]
    keys = qkv[:, width : 2 * width]
    values = qkv[:, 2 * width :]
    query_blocks = query.reshape(blocks_n, BLOCK, width)
    row_blocks = row_ids.reshape(blocks_n, BLOCK)

    def forward_block(entry):
        return attend_forward(entry[0], keys, values, entry[1], row_ids)

    mixed, log_sums = lax.map(forward_block, (query_blocks, row_blocks))
    mixed = mixed.reshape(rows_n, width).astype(jnp.bfloat16)
    middle = tokens_f + jnp.dot(mixed, full_out, preferred_element_type=jnp.float32) + shifts[3]
    normed_two_f, second_pull = jax.vjp(layer_norm, middle, gains[1], shifts[4])
    normed_two = normed_two_f.astype(jnp.bfloat16)
    upper = jnp.dot(normed_two, full_up, preferred_element_type=jnp.float32) + full_bias_up.astype(
        jnp.float32
    )
    hidden_f, gelu_pull = jax.vjp(gelu_tanh, upper)
    hidden = hidden_f.astype(jnp.bfloat16)
    block_out = (
        middle + jnp.dot(hidden, full_down, preferred_element_type=jnp.float32) + shifts[5]
    ).astype(jnp.bfloat16)
    back_qkv, back_out, back_up, back_down = full_qkv, full_out, full_up, full_down
    grad_out = cotangent.astype(jnp.float32)
    grad_shift_down = jnp.sum(grad_out, axis=0)
    grad_down = contract_rows(hidden, cotangent)
    d_hidden = contract_cols(cotangent, back_down)
    d_up = gelu_pull(d_hidden)[0].astype(jnp.bfloat16)
    grad_up = contract_rows(normed_two, d_up)
    grad_bias_up = jnp.sum(d_up, axis=0, dtype=jnp.float32)
    d_normed_two = contract_cols(d_up, back_up)
    d_middle_norm, grad_gain_two, grad_shift_two = second_pull(d_normed_two)
    d_middle = grad_out + d_middle_norm
    grad_shift_out = jnp.sum(d_middle, axis=0)
    d_middle_low = d_middle.astype(jnp.bfloat16)
    grad_out_proj = contract_rows(mixed, d_middle_low)
    d_mixed = contract_cols(d_middle_low, back_out).astype(jnp.bfloat16)
    d_blocks = d_mixed.reshape(blocks_n, BLOCK, width)

    def backward_step(carry, entry):
        d_query, d_keys, d_values = attend_backward(
            entry[0], keys, values, entry[1], row_ids, entry[2], entry[3]
        )
        return ((carry[0] + d_keys, carry[1] + d_values), d_query)

    empty = jnp.zeros((rows_n, width), jnp.float32)
    (d_keys, d_values), d_query = lax.scan(
        backward_step, (empty, empty), (query_blocks, row_blocks, log_sums, d_blocks)
    )
    d_query = d_query.reshape(rows_n, width)
    d_qkv = jnp.concatenate([d_query, d_keys, d_values], axis=1).astype(jnp.bfloat16)
    grad_qkv = contract_rows(normed, d_qkv)
    grad_bias_query = jnp.sum(d_qkv[:, :width], axis=0, dtype=jnp.float32)
    grad_bias_value = jnp.sum(d_qkv[:, 2 * width :], axis=0, dtype=jnp.float32)
    d_normed = contract_cols(d_qkv, back_qkv)
    d_tokens_norm, grad_gain_one, grad_shift_one = norm_pull(d_normed)
    d_inputs = d_middle + d_tokens_norm
    grad_gains = jnp.stack([grad_gain_one, grad_gain_two])
    grad_shifts = jnp.stack(
        [
            grad_shift_one,
            grad_bias_query,
            grad_bias_value,
            grad_shift_out,
            grad_shift_two,
            grad_shift_down,
        ]
    )
    small = (
        lax.psum_scatter(grad_gains, "fsdp", scatter_dimension=1, tiled=True),
        lax.psum_scatter(grad_shifts, "fsdp", scatter_dimension=1, tiled=True),
        lax.psum_scatter(grad_bias_up, "fsdp", scatter_dimension=0, tiled=True),
    )
    large = [g.astype(BF16) for g in (grad_down, grad_up, grad_out_proj, grad_qkv)]
    if fast:
        small = lax.psum(small, "dp")
        large = reduce_grads(*large)
    else:
        large = [lax.psum_scatter(g, "fsdp", scatter_dimension=0, tiled=True) for g in large]
        small, large = lax.psum((small, large), "dp")
    large = [g.astype(F32) for g in large]
    summed = (small[0], small[1], large[3], large[2], large[1], small[2], large[0])
    return (
        block_out,
        d_inputs,
        summed[0],
        summed[1],
        summed[2],
        summed[3],
        summed[4],
        summed[5],
        summed[6],
    )


def solution(mesh):
    fast = mesh.shape["fsdp"] == 8 and mesh.shape["dp"] == 4
    placed = (
        P(("fsdp", "dp"), None),
        P(("fsdp", "dp")),
        P(None, "fsdp"),
        P(None, "fsdp"),
        P("fsdp", None),
        P("fsdp", None),
        P("fsdp", None),
        P("fsdp"),
        P("fsdp", None),
        P(("fsdp", "dp"), None),
    )
    return jax.shard_map(
        functools.partial(per_device, fast),
        mesh=mesh,
        in_specs=placed,
        out_specs=(
            P(("fsdp", "dp"), None),
            P(("fsdp", "dp"), None),
            P(None, "fsdp"),
            P(None, "fsdp"),
            P("fsdp", None),
            P("fsdp", None),
            P("fsdp", None),
            P("fsdp"),
            P("fsdp", None),
        ),
        check_vma=False,
    )
```

```python
import functools
import math

import jax
import jax.numpy as jnp
from jax import lax
from jax.experimental import pallas as pl
from jax.experimental.pallas import tpu as pltpu
from jax.sharding import PartitionSpec as P

MESH = pl.DeviceIdType.MESH
F32 = jnp.float32
BF16 = jnp.bfloat16


class Place:
    def __init__(self):
        f = lax.axis_index("fsdp")
        d = lax.axis_index("dp")
        self.f, self.d = f, d
        self.z, self.x = f // 2, f % 2
        self.y, self.c = d // 2, d % 2

    def at(self, z=None, x=None, y=None, c=None):
        z = self.z if z is None else z
        x = self.x if x is None else x
        y = self.y if y is None else y
        c = self.c if c is None else c
        return (z * 2 + x, y * 2 + c)

    def z_to(self, k):
        return (self.z + k) % 4

    def z_from(self, k):
        return (self.z + 4 - k) % 4


def copy_to(src, dst, send, recv, device):
    return pltpu.make_async_remote_copy(
        src_ref=src, dst_ref=dst, send_sem=send, recv_sem=recv, device_id=device, device_id_type=MESH
    )


def greet(place):
    barrier = pltpu.get_barrier_semaphore()
    others = [place.at(z=place.z_to(k)) for k in (1, 2, 3)]
    others += [place.at(z=place.z_to(k), x=1 - place.x) for k in (0, 1, 2, 3)]
    others += [place.at(y=1 - place.y), place.at(c=1 - place.c)]
    for other in others:
        pl.semaphore_signal(barrier, inc=1, device_id=other, device_id_type=MESH)
    pl.semaphore_wait(barrier, len(others))


class Gather:
    def __init__(self, place, chunks, send, recv):
        self.p, self.chunks, self.send, self.recv = place, chunks, send, recv
        self.sent = []

    def view(self, k, f, start, width):
        src, full, rows, row, col = self.chunks[k]
        return full.at[pl.ds(pl.multiple_of(f * rows + row, 32), 96), pl.ds(pl.multiple_of(col + start, 128), width)]

    def own(self, k, start, width):
        src, full, rows, row, col = self.chunks[k]
        return src.at[pl.ds(row, 96), pl.ds(pl.multiple_of(col + start, 128), width)]

    def put(self, k, slot, src, dst, device):
        copy = copy_to(src, dst, self.send.at[k, slot], self.recv.at[k, slot], device)
        copy.start()
        self.sent.append(copy)

    def got(self, k, slot, dst):
        copy_to(dst, dst, self.send.at[k, slot], self.recv.at[k, slot], self.p.at(c=1 - self.p.c)).wait_recv()

    def ab(self):
        return self.p.c * 384 + self.p.y * 128

    def mine(self):
        return self.p.c * 384 + self.p.y * 256

    def theirs(self):
        return self.p.c * 384 + (1 - self.p.y) * 256

    def half(self):
        return self.p.c * 384

    def start(self, k):
        p = self.p
        src = self.own(k, self.ab(), 256)
        dst = self.view(k, p.f, self.ab(), 256)
        for hop in (1, 2, 3):
            self.put(k, hop - 1, src, dst, p.at(z=p.z_to(hop)))
        self.put(k, 3, src, dst, p.at(x=1 - p.x))

    def z_event(self, k, hop):
        p = self.p
        f = p.z_from(hop) * 2 + p.x
        ab = self.view(k, f, self.ab(), 256)
        self.got(k, hop - 1, ab)
        self.put(k, 3 + hop, ab, ab, p.at(x=1 - p.x))
        b = self.view(k, f, self.mine(), 128)
        self.put(k, 7 + hop - 1, b, b, p.at(y=1 - p.y))

    def x_event(self, k, hop):
        p = self.p
        f = p.z_from(hop) * 2 + 1 - p.x
        self.got(k, 3 + hop, self.view(k, f, self.ab(), 256))
        b = self.view(k, f, self.mine(), 128)
        self.put(k, 10 + hop, b, b, p.at(y=1 - p.y))

    def source(self, j):
        p = self.p
        return p.z_from(j + 1) * 2 + p.x if j < 3 else p.z_from(j - 3) * 2 + 1 - p.x

    def y_event(self, k, j):
        p = self.p
        f = self.source(j)
        self.got(k, 7 + j, self.view(k, f, self.theirs(), 128))
        h = self.view(k, f, self.half(), 384)
        self.put(k, 14 + j, h, h, p.at(c=1 - p.c))

    def c_event(self, k, j):
        p = self.p
        self.got(k, 14 + j, self.view(k, self.source(j), (1 - p.c) * 384, 384))

    def finish(self):
        for copy in self.sent:
            copy.wait_send()


class Reduce:
    def __init__(self, place, k, grads, bufs, final, send, recv):
        self.p, self.k, self.g, self.b, self.out = place, k, grads, bufs, final
        self.send, self.recv = send, recv
        self.sent = []
        self.slot_a = 3 * place.c + 1
        self.slot_b = 3 * place.c + 2 * place.y
        self.slot_o = 3 * place.c + 2 * (1 - place.y)

    def put(self, s, src, dst, device):
        copy = copy_to(src, dst, self.send.at[self.k, s], self.recv.at[self.k, s], device)
        copy.start()
        self.sent.append(copy)

    def got(self, s, dst):
        copy_to(dst, dst, self.send.at[self.k, s], self.recv.at[self.k, s], self.p.at(c=1 - self.p.c)).wait_recv()

    def add(self, dst, src):
        dst[...] = (dst[...].astype(F32) + src[...].astype(F32)).astype(BF16)

    def e0(self):
        p = self.p
        self.put(0, self.g.at[pl.ds(3 * (1 - p.c), 3)], self.b["c"], p.at(c=1 - p.c))

    def e1(self):
        p = self.p
        self.got(0, self.b["c"])
        base = 3 * p.c

        def body(i, _):
            s, z = i // 4, i % 4
            for x in (0, 1):
                self.add(self.g.at[base + s, z, x], self.b["c"].at[s, z, x])
            return 0

        lax.fori_loop(0, 12, body, 0)
        self.put(1, self.g.at[3 * p.c + 2 * (1 - p.y)], self.b["y"], p.at(y=1 - p.y))
        self.put(2, self.g.at[self.slot_a, :, 1 - p.x], self.b["xa"], p.at(x=1 - p.x))

    def x_add(self, slot, s, buf):
        p = self.p
        self.got(s, buf)

        def body(z, _):
            self.add(self.g.at[slot, z, p.x], buf.at[z])
            return 0

        lax.fori_loop(0, 4, body, 0)

    def z_put(self, slot, s, buf):
        p = self.p
        for hop in (1, 2, 3):
            z = p.z_to(hop)
            self.put(s + hop - 1, self.g.at[slot, z, p.x], buf.at[hop - 1], p.at(z=z))

    def z_sum(self, slot, s, buf):
        p = self.p
        total = self.g[slot, p.z, p.x].astype(F32)
        for hop in (1, 2, 3):
            self.got(s + hop - 1, buf.at[hop - 1])
            total = total + buf[hop - 1].astype(F32)
        return total.astype(BF16)

    def e2(self):
        self.x_add(self.slot_a, 2, self.b["xa"])
        self.z_put(self.slot_a, 3, self.b["za"])

    def e3(self):
        p = self.p
        self.got(1, self.b["y"])

        def body(z, _):
            for x in (0, 1):
                self.add(self.g.at[self.slot_b, z, x], self.b["y"].at[z, x])
            return 0

        lax.fori_loop(0, 4, body, 0)
        self.put(6, self.g.at[self.slot_b, :, 1 - p.x], self.b["xb"], p.at(x=1 - p.x))

    def e4(self):
        p = self.p
        self.b["pa"][...] = self.z_sum(self.slot_a, 3, self.b["za"])
        self.put(7, self.b["pa"], self.b["ya"], p.at(y=1 - p.y))

    def e5(self):
        self.x_add(self.slot_b, 6, self.b["xb"])
        self.z_put(self.slot_b, 8, self.b["zb"])

    def e6(self):
        p = self.p
        self.out[self.slot_b] = self.z_sum(self.slot_b, 8, self.b["zb"])
        self.put(11, self.out.at[self.slot_b], self.out.at[self.slot_b], p.at(y=1 - p.y))

    def e7(self):
        self.got(7, self.b["ya"])
        self.out[self.slot_a] = (self.b["pa"][...].astype(F32) + self.b["ya"][...].astype(F32)).astype(BF16)

    def e8(self):
        p = self.p
        self.got(11, self.out.at[self.slot_o])
        half = self.out.at[pl.ds(3 * p.c, 3)]
        self.put(12, half, half, p.at(c=1 - p.c))

    def e9(self):
        self.got(12, self.out.at[pl.ds(3 * (1 - self.p.c), 3)])

    def finish(self):
        for copy in self.sent:
            copy.wait_send()

    def events(self):
        return [self.e0, self.e1, self.e2, self.e3, self.e4, self.e5, self.e6, self.e7, self.e8, self.e9]


def reduce_bufs(r, w):
    v = lambda *lead: pltpu.VMEM((*lead, r, w), BF16)
    return dict(c=v(3, 4, 2), y=v(4, 2), xa=v(4), xb=v(4), za=v(3), zb=v(3), pa=v(), ya=v())


BUF_NAMES = ("c", "y", "xa", "xb", "za", "zb", "pa", "ya")


HEADS = 12
HEAD = 64
BLOCK = 512


norm_eps = 1e-05


def layer_norm(values, gain, shift):
    center = values - jnp.mean(values, axis=-1, keepdims=True)
    spread = jnp.mean(center * center, axis=-1, keepdims=True)
    return center * lax.rsqrt(spread + norm_eps) * gain + shift


def gelu_tanh(values):
    inner = math.sqrt(2.0 / math.pi) * (values + 0.044715 * values * values * values)
    return 0.5 * values * (1.0 + jnp.tanh(inner))


def contract_rows(left, right):
    return lax.dot_general(
        left, right, (((0,), (0,)), ((), ())), preferred_element_type=jnp.float32
    )


def contract_cols(left, right):
    return lax.dot_general(
        left, right, (((1,), (1,)), ((), ())), preferred_element_type=jnp.float32
    )


def split_heads(values):
    return values.reshape(values.shape[0], HEADS, values.shape[1] // HEADS)


def block_scores(query, keys, query_rows, key_rows):
    raw_scores = jnp.einsum(
        "qhd,khd->hqk", split_heads(query), split_heads(keys), preferred_element_type=jnp.float32
    )
    raw_scores = raw_scores * (1.0 / math.sqrt(HEAD))
    same_row = (query_rows[:, None] == key_rows[None, :])[None]
    return jnp.where(same_row, raw_scores, -1000000000.0)


def attend_forward(query, keys, values, query_rows, key_rows):
    scores = block_scores(query, keys, query_rows, key_rows)
    row_max = jnp.max(scores, axis=-1, keepdims=True)
    exponent = jnp.exp(scores - row_max)
    row_sum = jnp.sum(exponent, axis=-1, keepdims=True)
    attn_probs = (exponent / row_sum).astype(jnp.bfloat16)
    result = jnp.einsum(
        "hqk,khd->qhd", attn_probs, split_heads(values), preferred_element_type=jnp.float32
    )
    return (result.reshape(query.shape[0], -1), (row_max + jnp.log(row_sum))[..., 0])


def attend_backward(query, keys, values, query_rows, key_rows, log_sums, grad_out):
    scores = block_scores(query, keys, query_rows, key_rows)
    attn_probs = jnp.exp(scores - log_sums[..., None])
    probs_low = attn_probs.astype(jnp.bfloat16)
    grad_heads = split_heads(grad_out)
    d_values = jnp.einsum("hqk,qhd->khd", probs_low, grad_heads, preferred_element_type=jnp.float32)
    d_probs = jnp.einsum(
        "qhd,khd->hqk", grad_heads, split_heads(values), preferred_element_type=jnp.float32
    )
    inner = jnp.sum(attn_probs * d_probs, axis=-1, keepdims=True)
    d_scores = (attn_probs * (d_probs - inner)).astype(jnp.bfloat16)
    scale = 1.0 / math.sqrt(HEAD)
    d_query = (
        jnp.einsum("hqk,khd->qhd", d_scores, split_heads(keys), preferred_element_type=jnp.float32)
        * scale
    )
    d_keys = (
        jnp.einsum("hqk,qhd->khd", d_scores, split_heads(query), preferred_element_type=jnp.float32)
        * scale
    )
    return (
        d_query.reshape(query.shape[0], -1),
        d_keys.reshape(keys.shape[0], -1),
        d_values.reshape(keys.shape[0], -1),
    )


def per_device(inputs, row_ids, ln_gains, biases, w_qkv, w_out, w_up, bias_up, w_down, cotangent):
    gathered = (
        lax.all_gather(ln_gains, "fsdp", axis=1, tiled=True),
        lax.all_gather(biases, "fsdp", axis=1, tiled=True),
        lax.all_gather(w_qkv, "fsdp", axis=0, tiled=True),
        lax.all_gather(w_out, "fsdp", axis=0, tiled=True),
        lax.all_gather(w_up, "fsdp", axis=0, tiled=True),
        lax.all_gather(bias_up, "fsdp", axis=0, tiled=True),
        lax.all_gather(w_down, "fsdp", axis=0, tiled=True),
    )
    gains = gathered[0].astype(jnp.float32)
    shifts = gathered[1].astype(jnp.float32)
    full_qkv, full_out, full_up, full_bias_up, full_down = (
        gathered[2],
        gathered[3],
        gathered[4],
        gathered[5],
        gathered[6],
    )
    width = full_out.shape[0]
    rows_n = inputs.shape[0]
    blocks_n = rows_n // BLOCK
    tokens_f = inputs.astype(jnp.float32)
    normed_f, norm_pull = jax.vjp(layer_norm, tokens_f, gains[0], shifts[0])
    normed = normed_f.astype(jnp.bfloat16)
    qkv_bias = jnp.concatenate([shifts[1], jnp.zeros_like(shifts[1]), shifts[2]])
    qkv = (jnp.dot(normed, full_qkv, preferred_element_type=jnp.float32) + qkv_bias).astype(
        jnp.bfloat16
    )
    query = qkv[:, :width]
    keys = qkv[:, width : 2 * width]
    values = qkv[:, 2 * width :]
    query_blocks = query.reshape(blocks_n, BLOCK, width)
    row_blocks = row_ids.reshape(blocks_n, BLOCK)

    def forward_block(entry):
        return attend_forward(entry[0], keys, values, entry[1], row_ids)

    mixed, log_sums = lax.map(forward_block, (query_blocks, row_blocks))
    mixed = mixed.reshape(rows_n, width).astype(jnp.bfloat16)
    middle = tokens_f + jnp.dot(mixed, full_out, preferred_element_type=jnp.float32) + shifts[3]
    normed_two_f, second_pull = jax.vjp(layer_norm, middle, gains[1], shifts[4])
    normed_two = normed_two_f.astype(jnp.bfloat16)
    upper = jnp.dot(normed_two, full_up, preferred_element_type=jnp.float32) + full_bias_up.astype(
        jnp.float32
    )
    hidden_f, gelu_pull = jax.vjp(gelu_tanh, upper)
    hidden = hidden_f.astype(jnp.bfloat16)
    block_out = (
        middle + jnp.dot(hidden, full_down, preferred_element_type=jnp.float32) + shifts[5]
    ).astype(jnp.bfloat16)
    back_qkv, back_out, back_up, back_down = full_qkv, full_out, full_up, full_down
    grad_out = cotangent.astype(jnp.float32)
    grad_shift_down = jnp.sum(grad_out, axis=0)
    grad_down = contract_rows(hidden, cotangent)
    d_hidden = contract_cols(cotangent, back_down)
    d_up = gelu_pull(d_hidden)[0].astype(jnp.bfloat16)
    grad_up = contract_rows(normed_two, d_up)
    grad_bias_up = jnp.sum(d_up, axis=0, dtype=jnp.float32)
    d_normed_two = contract_cols(d_up, back_up)
    d_middle_norm, grad_gain_two, grad_shift_two = second_pull(d_normed_two)
    d_middle = grad_out + d_middle_norm
    grad_shift_out = jnp.sum(d_middle, axis=0)
    d_middle_low = d_middle.astype(jnp.bfloat16)
    grad_out_proj = contract_rows(mixed, d_middle_low)
    d_mixed = contract_cols(d_middle_low, back_out).astype(jnp.bfloat16)
    d_blocks = d_mixed.reshape(blocks_n, BLOCK, width)

    def backward_step(carry, entry):
        d_query, d_keys, d_values = attend_backward(
            entry[0], keys, values, entry[1], row_ids, entry[2], entry[3]
        )
        return ((carry[0] + d_keys, carry[1] + d_values), d_query)

    empty = jnp.zeros((rows_n, width), jnp.float32)
    (d_keys, d_values), d_query = lax.scan(
        backward_step, (empty, empty), (query_blocks, row_blocks, log_sums, d_blocks)
    )
    d_query = d_query.reshape(rows_n, width)
    d_qkv = jnp.concatenate([d_query, d_keys, d_values], axis=1).astype(jnp.bfloat16)
    grad_qkv = contract_rows(normed, d_qkv)
    grad_bias_query = jnp.sum(d_qkv[:, :width], axis=0, dtype=jnp.float32)
    grad_bias_value = jnp.sum(d_qkv[:, 2 * width :], axis=0, dtype=jnp.float32)
    d_normed = contract_cols(d_qkv, back_qkv)
    d_tokens_norm, grad_gain_one, grad_shift_one = norm_pull(d_normed)
    d_inputs = d_middle + d_tokens_norm
    grad_gains = jnp.stack([grad_gain_one, grad_gain_two])
    grad_shifts = jnp.stack(
        [
            grad_shift_one,
            grad_bias_query,
            grad_bias_value,
            grad_shift_out,
            grad_shift_two,
            grad_shift_down,
        ]
    )
    sums = (grad_gains, grad_shifts, grad_qkv, grad_out_proj, grad_up, grad_bias_up, grad_down)
    owned = []
    for index, grad in enumerate(sums):
        kept = grad.astype(BF16) if index in (2, 3, 4, 6) else grad
        owned.append(lax.psum_scatter(kept, "fsdp", scatter_dimension=1 if index < 2 else 0, tiled=True))
    summed = [v.astype(F32) for v in lax.psum(tuple(owned), "dp")]
    return (
        block_out,
        d_inputs,
        summed[0],
        summed[1],
        summed[2],
        summed[3],
        summed[4],
        summed[5],
        summed[6],
    )


SETS = (0, 1, 2, 3, 4, 5, 6, 7, 0, 1, 2, 3)
TILE = 256


def dot_nn(a, b):
    return jnp.dot(a, b, preferred_element_type=F32)


def dot_nt(a, b):
    return contract_cols(a, b)


def dot_tn(a, b):
    return contract_rows(a, b)


def norm_parts(values):
    center = values - jnp.mean(values, axis=-1, keepdims=True)
    spread = jnp.mean(center * center, axis=-1, keepdims=True)
    scale = lax.rsqrt(spread + norm_eps)
    return center * scale, scale


def norm_back(normal, scale, gain, grad):
    scaled = grad * gain
    inner = jnp.mean(scaled * normal, axis=-1, keepdims=True)
    return scale * (scaled - jnp.mean(scaled, axis=-1, keepdims=True) - normal * inner)


def col_sum(values):
    return jnp.sum(values, axis=0, keepdims=True)


def lane_masks():
    lane = lax.broadcasted_iota(jnp.int32, (TILE, 256), 1) // HEAD
    return [lane == h for h in range(4)]


def head_probs(query, keys, cap):
    scores = jnp.minimum(dot_nt(query, keys), cap)
    exponent = jnp.exp(scores - jnp.max(scores, axis=-1, keepdims=True))
    return exponent * (1.0 / jnp.sum(exponent, axis=-1, keepdims=True))


def score_cap(pen_ref, block):
    top = lax.broadcasted_iota(jnp.int32, (TILE, TILE), 0) < TILE // 2
    left = lax.broadcasted_iota(jnp.int32, (TILE, TILE), 1) < TILE // 2
    return jnp.where(top == left, 3.0e38, pen_ref[pl.ds(block, 1), :])


class SmallReduce:
    def __init__(self, place, mine, bufs, send, recv):
        self.p, self.g, self.b, self.send, self.recv = place, mine, bufs, send, recv
        self.sent = []

    def put(self, s, src, dst, device):
        copy = copy_to(src, dst, self.send.at[s], self.recv.at[s], device)
        copy.start()
        self.sent.append(copy)

    def got(self, s, dst):
        copy_to(dst, dst, self.send.at[s], self.recv.at[s], self.p.at(c=1 - self.p.c)).wait_recv()

    def e0(self):
        self.put(0, self.g, self.b[0], self.p.at(c=1 - self.p.c))

    def e1(self):
        p = self.p
        self.got(0, self.b[0])
        self.b[1][...] = self.g[...] + self.b[0][...]
        self.put(1, self.b[1].at[:, 1 - p.x], self.b[2], p.at(x=1 - p.x))

    def e2(self):
        p = self.p
        self.got(1, self.b[2])
        self.b[3][...] = self.b[1][:, p.x] + self.b[2][...]
        for hop in (1, 2, 3):
            z = p.z_to(hop)
            self.put(1 + hop, self.b[3].at[z], self.b[4].at[hop - 1], p.at(z=z))

    def e3(self):
        p = self.p
        total = self.b[3][p.z]
        for hop in (1, 2, 3):
            self.got(1 + hop, self.b[4].at[hop - 1])
            total = total + self.b[4][hop - 1]
        self.b[5][...] = total
        self.put(5, self.b[5], self.b[6], p.at(y=1 - p.y))

    def e4(self, out):
        self.got(5, self.b[6])
        out[...] = self.b[5][...] + self.b[6][...]

    def finish(self):
        for copy in self.sent:
            copy.wait_send()


SMALL_BUFS = ((4, 2), (4, 2), (4,), (4,), (3,), (), ())


def block_kernel(
    x_ref, pen_ref, small_ref, q_ref, o_ref, u_ref, d_ref, c_ref,
    out_ref, din_ref, gs_ref, gq_ref, go_ref, gu_ref, gd_ref,
    wq, wo, wu, wd, cot, n1, qkv, mix, mid, n2, hid, gp, grads, fin,
    par, bup, small, sums, sum_up, sgrad, bufs, sbufs,
    ag_send, ag_recv, rs_send, rs_recv, sm_send, sm_recv, sr_send, sr_recv, local, outs,
):
    p = Place()
    chunks = [(q_ref, wq, 96, 0, 768 * j) for j in range(3)]
    chunks += [(o_ref, wo, 96, 0, 0)]
    chunks += [(u_ref, wu, 96, 0, 768 * j) for j in range(4)]
    chunks += [(d_ref, wd, 384, 96 * j, 0) for j in range(4)]
    gather = Gather(p, chunks, ag_send, ag_recv)
    rows_of = lambda i: pl.ds(pl.multiple_of(i * TILE, TILE), TILE)

    load_x = pltpu.make_async_copy(x_ref, n2, local.at[0])
    load_x.start()
    load_c = pltpu.make_async_copy(c_ref, cot, local.at[1])
    load_c.start()
    own_small = pltpu.make_async_copy(small_ref, small.at[p.f], local.at[2])
    own_small.start()
    owns = []
    for i, (src, dst, rows) in enumerate(((q_ref, wq, 96), (o_ref, wo, 96), (u_ref, wu, 96), (d_ref, wd, 384))):
        copy = pltpu.make_async_copy(src, dst.at[pl.ds(pl.multiple_of(p.f * rows, 32), rows)], local.at[3 + i])
        copy.start()
        owns.append(copy)
    greet(p)
    small_sent = []
    for i in range(1, 8):
        f = (p.f + i) % 8
        copy = copy_to(small_ref, small.at[p.f], sm_send.at[i - 1], sm_recv.at[i - 1], (f, p.d))
        copy.start()
        small_sent.append(copy)
    for k in range(3):
        gather.start(k)

    def z_events(k):
        return [functools.partial(gather.z_event, k, hop) for hop in (1, 2, 3)]

    def x_events(k):
        return [functools.partial(gather.x_event, k, hop) for hop in (0, 1, 2, 3)]

    def y_events(k):
        return [functools.partial(gather.y_event, k, j) for j in range(7)]

    def c_events(k):
        return [functools.partial(gather.c_event, k, j) for j in range(7)]

    def run(events):
        for event in events:
            event()

    sums[...] = jnp.zeros_like(sums)
    sum_up[...] = jnp.zeros_like(sum_up)
    own_small.wait()
    for i in range(1, 8):
        f = (p.f + 8 - i) % 8
        copy_to(small.at[f], small.at[f], sm_send.at[i - 1], sm_recv.at[i - 1], (f, p.d)).wait_recv()
    gathered = jnp.zeros((16, 768), F32)
    for f in range(8):
        lane = lax.broadcasted_iota(jnp.int32, (128, 768), 0)
        column = lax.broadcasted_iota(jnp.int32, (128, 768), 1)
        pick = jnp.where((column == lane + 96 * f) & (lane < 96), 1.0, 0.0).astype(BF16)
        gathered = gathered + dot_nn(small[f].astype(BF16), pick)
        for r in range(3):
            bup[0:1, 384 * f + 128 * r : 384 * f + 128 * r + 128] = small[f, 8 + r : 9 + r, :]
    par[...] = gathered
    load_x.wait()

    def first_norm(i, _):
        rows = rows_of(i)
        values = n2[rows, :].astype(F32)
        normal, _scale = norm_parts(values)
        n1[rows, :] = (normal * par[0:1, :] + par[2:3, :]).astype(BF16)
        mid[rows, :] = values
        return 0

    lax.fori_loop(0, 4, first_norm, 0)
    for k in range(3, 12):
        pass
    run(z_events(0))
    run(x_events(0) + z_events(1))
    run(y_events(0) + x_events(1) + z_events(2))
    for k in (3, 4, 5):
        gather.start(k)
    for copy in owns:
        copy.wait()
    run(c_events(0) + y_events(1) + x_events(2))

    def project(part):
        columns = pl.ds(768 * part, 768)
        bias = par[(3, None, 4)[part] : (4, None, 5)[part], :] if part != 1 else None

        def body(i, _):
            rows = rows_of(i)
            value = dot_nn(n1[rows, :], wq[:, columns])
            if bias is not None:
                value = value + bias
            qkv[rows, columns] = value.astype(BF16)
            return 0

        lax.fori_loop(0, 4, body, 0)

    project(0)
    run(c_events(1) + y_events(2))
    project(1)
    run(c_events(2))
    project(2)

    def attend(g, queue):
        def body(i, _):
            rows = rows_of(i)
            masks = lane_masks()
            cap = score_cap(pen_ref, i)
            query = qkv[rows, 256 * g : 256 * g + 256] * BF16(0.125)
            keys = qkv[rows, 768 + 256 * g : 1024 + 256 * g]
            values = qkv[rows, 1536 + 256 * g : 1792 + 256 * g]
            zero = jnp.zeros_like(query)
            probs, parts = [], []
            for h in range(4):
                probs.append(head_probs(jnp.where(masks[h], query, zero), keys, cap).astype(BF16))
                parts.append(jnp.where(masks[h], values, zero))
            result = dot_nn(jnp.concatenate(probs, axis=1), jnp.concatenate(parts, axis=0))
            mix[rows, 256 * g : 256 * g + 256] = result.astype(BF16)
            return 0

        for start in (0, 2):
            lax.fori_loop(start, start + 2, body, 0)
            run(queue.pop(0) if queue else [])

    for k in (6, 7, 8):
        gather.start(k)
    queue = [
        z_events(3) + x_events(3) + z_events(4),
        x_events(4) + y_events(3) + z_events(5),
        x_events(5) + y_events(4),
        z_events(6) + y_events(5) + c_events(3) + c_events(4),
        x_events(6) + z_events(7) + c_events(5),
        y_events(6) + x_events(7),
    ]
    for g in range(3):
        attend(g, queue)
    for k in (9, 10, 11):
        gather.start(k)

    def out_project(i, _):
        rows = rows_of(i)
        value = mid[rows, :] + dot_nn(mix[rows, :], wo[...]) + par[5:6, :]
        mid[rows, :] = value
        normal, _scale = norm_parts(value)
        n2[rows, :] = (normal * par[1:2, :] + par[6:7, :]).astype(BF16)
        return 0

    lax.fori_loop(0, 4, out_project, 0)
    run(z_events(8) + y_events(7) + c_events(6))

    root = math.sqrt(2.0 / math.pi)

    def up_project(j):
        def body(i, _):
            rows = rows_of(i)
            for part in range(3):
                columns = slice(768 * j + 256 * part, 768 * j + 256 * part + 256)
                u = dot_nn(n2[rows, :], wu[:, columns]) + bup[0:1, columns]
                square = u * u
                t = jnp.tanh(root * u * (1.0 + 0.044715 * square))
                half = 0.5 * (1.0 + t)
                slope = half + (0.5 * root) * u * (1.0 - t * t) * (1.0 + (3 * 0.044715) * square)
                hid[rows, columns] = (u * half).astype(BF16)
                gp[rows, columns] = slope.astype(BF16)
            return 0

        lax.fori_loop(0, 4, body, 0)

    up_project(0)
    run(x_events(8) + z_events(9))
    up_project(1)
    run(c_events(7) + y_events(8) + x_events(9))
    up_project(2)
    run(z_events(10) + y_events(9) + x_events(10))
    up_project(3)
    run(z_events(11) + c_events(8) + y_events(10))

    load_c.wait()

    def down_grad(f, _):
        z, x = f // 2, f % 2
        value = dot_tn(hid[:, pl.ds(pl.multiple_of(f * 384, 128), 384)], cot[...]).astype(BF16)
        for j in range(4):
            for s in range(6):
                grads[j, s, z, x] = value[96 * j : 96 * j + 96, 128 * s : 128 * s + 128]
        return 0

    lax.fori_loop(0, 4, down_grad, 0)
    run(x_events(11) + c_events(9))
    lax.fori_loop(4, 8, down_grad, 0)
    run(y_events(11) + c_events(10))

    reduces = []
    for k in range(12):
        reduces.append(
            Reduce(p, k, grads.at[SETS[k]], {n: r.at[SETS[k]] for n, r in bufs.items()}, fin.at[k], rs_send, rs_recv)
        )
    stores = []

    def store(k):
        for s in range(6):
            if k < 4:
                dst = gd_ref.at[pl.ds(96 * k, 96), pl.ds(128 * s, 128)]
            elif k < 8:
                dst = gu_ref.at[:, pl.ds(768 * (k - 4) + 128 * s, 128)]
            elif k == 8:
                dst = go_ref.at[:, pl.ds(128 * s, 128)]
            else:
                dst = gq_ref.at[:, pl.ds((s // 2) * 768 + 256 * (k - 9) + 128 * (s % 2), 128)]
            copy = pltpu.make_async_copy(fin.at[k, s], dst, outs.at[k, s])
            copy.start()
            stores.append(copy)

    first = FIRST
    done = {"step": 0, "left": [list(range(10)) for _ in range(12)]}

    def advance(steps=1):
        for _ in range(steps):
            t = done["step"]
            for stage in range(9, -1, -1):
                for k in range(12):
                    if first[k] + stage == t:
                        reduces[k].events()[stage]()
                        if stage == 9:
                            store(k)
            done["step"] += 1

    advance()
    run(c_events(11))

    def hidden_back(j):
        def body(i, _):
            rows = rows_of(i)
            columns = slice(768 * j, 768 * j + 768)
            value = dot_nt(cot[rows, :], wd[columns, :])
            value = (value * gp[rows, columns].astype(F32)).astype(BF16)
            gp[rows, columns] = value
            sum_up[0:1, columns] += col_sum(value.astype(F32))
            return 0

        lax.fori_loop(0, 4, body, 0)

    for j in range(4):
        hidden_back(j)
        advance()

    def block_result(i, _):
        rows = rows_of(i)
        value = mid[rows, :] + dot_nn(hid[rows, :], wd[...]) + par[7:8, :]
        hid[rows, 0:768] = value.astype(BF16)
        return 0

    lax.fori_loop(0, 2, block_result, 0)
    advance()
    lax.fori_loop(2, 4, block_result, 0)
    advance()
    result_out = pltpu.make_async_copy(hid.at[:, pl.ds(0, 768)], out_ref, local.at[7])
    result_out.start()
    again_x = pltpu.make_async_copy(x_ref, hid.at[:, pl.ds(768, 768)], local.at[8])
    again_x.start()

    def store_grads(k, value):
        for s in range(6):
            grads[SETS[k], s] = value[:, 128 * s : 128 * s + 128].reshape(4, 2, 96, 128)

    for j in range(4):
        store_grads(4 + j, dot_tn(n2[...], gp[:, 768 * j : 768 * j + 768]).astype(BF16))
        advance()

    def second_back(i, _):
        rows = rows_of(i)
        grad = dot_nt(gp[rows, :], wu[...])
        normal, scale = norm_parts(mid[rows, :])
        sums[1:2, :] += col_sum(grad * normal)
        sums[6:7, :] += col_sum(grad)
        outer = cot[rows, :].astype(F32)
        sums[7:8, :] += col_sum(outer)
        value = outer + norm_back(normal, scale, par[1:2, :], grad)
        sums[5:6, :] += col_sum(value)
        mid[rows, :] = value
        n2[rows, :] = value.astype(BF16)
        return 0

    lax.fori_loop(0, 2, second_back, 0)
    advance()
    lax.fori_loop(2, 4, second_back, 0)
    advance()
    for k in range(4):
        reduces[k].finish()
    store_grads(8, dot_tn(mix[...], n2[...]).astype(BF16))
    advance()

    def mixed_back(i, _):
        rows = rows_of(i)
        mix[rows, :] = dot_nt(n2[rows, :], wo[...]).astype(BF16)
        return 0

    lax.fori_loop(0, 4, mixed_back, 0)

    def attend_back(g, i):
        rows = rows_of(i)
        masks = lane_masks()
        cap = score_cap(pen_ref, i)
        cols = [slice(768 * part + 256 * g, 768 * part + 256 * g + 256) for part in range(3)]
        query = qkv[rows, cols[0]] * BF16(0.125)
        keys = qkv[rows, cols[1]]
        values = qkv[rows, cols[2]]
        grad = mix[rows, 256 * g : 256 * g + 256]
        zero = jnp.zeros_like(query)
        probs, scores, queries, key_parts, grad_parts = [], [], [], [], []
        for h in range(4):
            q_h = jnp.where(masks[h], query, zero)
            g_h = jnp.where(masks[h], grad, zero)
            prob = head_probs(q_h, keys, cap)
            d_prob = dot_nt(g_h, values)
            inner = jnp.sum(prob * d_prob, axis=-1, keepdims=True)
            probs.append(prob.astype(BF16))
            scores.append((prob * (d_prob - inner)).astype(BF16))
            queries.append(q_h)
            key_parts.append(jnp.where(masks[h], keys, zero))
            grad_parts.append(g_h)
        d_query = dot_nn(jnp.concatenate(scores, axis=1), jnp.concatenate(key_parts, axis=0)) * 0.125
        d_keys = dot_tn(jnp.concatenate(scores, axis=0), jnp.concatenate(queries, axis=0))
        d_values = dot_tn(jnp.concatenate(probs, axis=0), jnp.concatenate(grad_parts, axis=0))
        low = [v.astype(BF16) for v in (d_query, d_keys, d_values)]
        for part in range(3):
            qkv[rows, cols[part]] = low[part]
        sums[3:4, 256 * g : 256 * g + 256] += col_sum(low[0].astype(F32))
        sums[4:5, 256 * g : 256 * g + 256] += col_sum(low[2].astype(F32))
        return 0

    for g in range(3):
        for start in (0, 2):
            lax.fori_loop(start, start + 2, lambda i, _: attend_back(g, i), 0)
            advance()
        for part in range(3):
            columns = slice(768 * part + 256 * g, 768 * part + 256 * g + 256)
            value = dot_tn(n1[...], qkv[:, columns]).astype(BF16)
            for half in range(2):
                grads[SETS[9 + g], 2 * part + half] = value[:, 128 * half : 128 * half + 128].reshape(4, 2, 96, 128)
        advance()

    again_x.wait()

    def first_back(i, _):
        rows = rows_of(i)
        grad = dot_nt(qkv[rows, :], wq[...])
        normal, scale = norm_parts(hid[rows, 768:1536].astype(F32))
        sums[0:1, :] += col_sum(grad * normal)
        sums[2:3, :] += col_sum(grad)
        mid[rows, :] = mid[rows, :] + norm_back(normal, scale, par[0:1, :], grad)
        return 0

    lax.fori_loop(0, 2, first_back, 0)
    advance()
    lax.fori_loop(2, 4, first_back, 0)
    input_out = pltpu.make_async_copy(mid, din_ref, local.at[9])
    input_out.start()

    every = sums[...]
    for f in range(8):
        turned = every if f == 0 else pltpu.roll(every, 768 - 96 * f, 1)
        sgrad[f // 2, f % 2, 0:8, :] = turned[:, 0:128]
        for r in range(3):
            sgrad[f // 2, f % 2, 8 + r : 9 + r, :] = sum_up[0:1, 384 * f + 128 * r : 384 * f + 128 * r + 128]
        sgrad[f // 2, f % 2, 11:16, :] = jnp.zeros((5, 128), F32)
    tiny = SmallReduce(p, sgrad, sbufs, sr_send, sr_recv)
    tiny.e0()
    advance()
    tiny.e1()
    advance()
    tiny.e2()
    advance()
    tiny.e3()
    advance()
    tiny.e4(gs_ref)
    while done["step"] <= max(first) + 9:
        advance()
    for copy in small_sent:
        copy.wait_send()
    gather.finish()
    for k in range(4, 12):
        reduces[k].finish()
    tiny.finish()
    result_out.wait()
    input_out.wait()
    for copy in stores:
        copy.wait()


FIRST = (0, 1, 2, 3, 7, 8, 9, 10, 13, 16, 19, 22)


def fused_block(x, penalty, small, w_qkv, w_out, w_up, w_down, cotangent):
    hbm = pl.BlockSpec(memory_space=pl.ANY)
    vmem = pl.BlockSpec(memory_space=pltpu.VMEM)
    tokens, width = x.shape
    hidden = w_up.shape[1]
    big = lambda *s: pltpu.VMEM(s, BF16)
    dma = pltpu.SemaphoreType.DMA
    unit = lambda lead: pltpu.VMEM((8, *lead, 96, 128), BF16)
    shapes = reduce_bufs(96, 128)
    return pl.pallas_call(
        block_kernel,
        out_shape=[
            jax.ShapeDtypeStruct((tokens, width), BF16),
            jax.ShapeDtypeStruct((tokens, width), F32),
            jax.ShapeDtypeStruct((16, 128), F32),
            jax.ShapeDtypeStruct(w_qkv.shape, BF16),
            jax.ShapeDtypeStruct(w_out.shape, BF16),
            jax.ShapeDtypeStruct(w_up.shape, BF16),
            jax.ShapeDtypeStruct(w_down.shape, BF16),
        ],
        in_specs=[hbm, vmem, hbm, hbm, hbm, hbm, hbm, hbm],
        out_specs=[hbm, hbm, vmem, hbm, hbm, hbm, hbm],
        scratch_shapes=[
            big(width, 3 * width),
            big(width, width),
            big(width, hidden),
            big(hidden, width),
            big(tokens, width),
            big(tokens, width),
            big(tokens, 3 * width),
            big(tokens, width),
            pltpu.VMEM((tokens, width), F32),
            big(tokens, width),
            big(tokens, hidden),
            big(tokens, hidden),
            big(8, 6, 4, 2, 96, 128),
            big(12, 6, 96, 128),
            pltpu.VMEM((16, width), F32),
            pltpu.VMEM((8, hidden), F32),
            pltpu.VMEM((8, 16, 128), F32),
            pltpu.VMEM((8, width), F32),
            pltpu.VMEM((8, hidden), F32),
            pltpu.VMEM((4, 2, 16, 128), F32),
            {n: pltpu.VMEM((8, *shapes[n].shape), BF16) for n in BUF_NAMES},
            [pltpu.VMEM((*lead, 16, 128), F32) for lead in SMALL_BUFS],
            dma((12, 21)),
            dma((12, 21)),
            dma((12, 13)),
            dma((12, 13)),
            dma((7,)),
            dma((7,)),
            dma((6,)),
            dma((6,)),
            dma((10,)),
            dma((12, 6)),
        ],
        compiler_params=pltpu.CompilerParams(
            collective_id=0, has_side_effects=True, vmem_limit_bytes=67043328
        ),
        name="block",
    )(x, penalty, small, w_qkv, w_out, w_up, w_down, cotangent)


def fast_device(inputs, row_ids, ln_gains, biases, w_qkv, w_out, w_up, bias_up, w_down, cotangent):
    starts = row_ids.reshape(-1, 2, TILE // 2)[:, :, 0]
    penalty = jnp.where(starts[:, 0] == starts[:, 1], 3.0e38, -1.0e9).astype(F32)
    penalty = jnp.broadcast_to(penalty[:, None], (penalty.shape[0], TILE))
    both = jnp.concatenate([ln_gains, biases], axis=0).astype(F32)
    both = jnp.pad(both, ((0, 0), (0, 128 - both.shape[1])))
    small = jnp.concatenate([both, jnp.pad(bias_up.astype(F32).reshape(3, 128), ((0, 5), (0, 0)))], axis=0)
    block_out, d_inputs, gs, gq, go, gu, gd = fused_block(
        inputs, penalty, small, w_qkv, w_out, w_up, w_down, cotangent
    )
    return (
        block_out,
        d_inputs,
        gs[0:2, 0:96],
        gs[2:8, 0:96],
        gq.astype(F32),
        go.astype(F32),
        gu.astype(F32),
        gs[8:11, :].reshape(-1),
        gd.astype(F32),
    )


def solution(mesh):
    fast = mesh.shape["fsdp"] == 8 and mesh.shape["dp"] == 4
    placed = (
        P(("fsdp", "dp"), None),
        P(("fsdp", "dp")),
        P(None, "fsdp"),
        P(None, "fsdp"),
        P("fsdp", None),
        P("fsdp", None),
        P("fsdp", None),
        P("fsdp"),
        P("fsdp", None),
        P(("fsdp", "dp"), None),
    )
    return jax.shard_map(
        fast_device if fast else per_device,
        mesh=mesh,
        in_specs=placed,
        out_specs=(
            P(("fsdp", "dp"), None),
            P(("fsdp", "dp"), None),
            P(None, "fsdp"),
            P(None, "fsdp"),
            P("fsdp", None),
            P("fsdp", None),
            P("fsdp", None),
            P("fsdp"),
            P("fsdp", None),
        ),
        check_vma=False,
    )
```
